512 devices in a mesh: section: 4 (over x_hi, core), seq: 128 (over z, y, x_lo).
Axes of the slice: x: 4 (x_hi: 2, x_lo: 2; x = x_hi * 2 + x_lo), y: 8, z: 8, core: 2. Of those that a mesh axis runs over, the one named last changes fastest.
Arguments:
- hidden: bfloat16 [2, 16384, 2688], P(None, 'seq'), may hold values from -6 to 6
- lengths: int32 [2], replicated, may hold values from 8192 to 16384, as said below
- reward_pos: int32 [2], replicated, may hold values from 8064 to 16383, as said below
- in_gain: bfloat16 [2688], P('seq'), may hold values from 0.099609375 to 1.8984375
- w_query: bfloat16 [2688, 2048], P('seq', 'section'), may hold values from -0.077151675 to 0.077151675
- w_key: bfloat16 [2688, 1024], P('seq', 'section'), may hold values from -0.077151675 to 0.077151675
- w_value: bfloat16 [2688, 1024], P('seq', 'section'), may hold values from -0.125 to 0.125
- query_gain: float32 [128], replicated, may hold values from 0.6 to 7
- key_gain: float32 [128], replicated, may hold values from 0.6 to 7
- w_out: bfloat16 [2048, 2688], P('section', 'seq'), may hold values from -0.125 to 0.125
- post_gain: bfloat16 [2688], P('seq'), may hold values from 0.099609375 to 1.8984375
- final_gain: bfloat16 [2688], P('seq'), may hold values from 0.099609375 to 1.8984375
- value_head: bfloat16 [2688], P('seq'), may hold values from -0.125 to 0.125
Outputs:
- token_values: float32 [2, 16384], P(None, 'seq')
- reward: float32 [2], replicated
The draws below stay inside these ranges and needn't reach their ends.
Inputs may be any that keep to these rules, and one draw needn't show every extreme that they name: `lengths`: in every draw at least one micro-batch has all 16384 tokens valid. reward_pos[m] lies among the last 128 valid tokens of micro-batch m.
All inputs are finite; a program needn't handle non-finite values.
Results may differ from the reference program's by a relative error of at most 0.01.
Values may be sent and summed in bfloat16 or wider, within the bound.
No kernel may reach another device: no remote copies, remote signals or barrier semaphores. Data moves between devices by JAX's collectives and lax.ppermute only.
A program may use at most 64 MiB of HBM per device.

```python
import jax
import jax.numpy as jnp
from jax import lax

D = 2688
HD = 128
GROUP = 2
WINDOW = 1024
MICRO = 2
TOK_DEV = 128
KVH = 8
TOKENS = 16384
N_SEQ = 128


def weight_pair(key):
    base_key = jax.random.fold_in(key, 11)
    query_part = jax.random.truncated_normal(jax.random.fold_in(base_key, 1), -4.0, 4.0, (D, GROUP * HD * KVH), jnp.float32) * D ** (-0.5)
    key_part = jax.random.truncated_normal(jax.random.fold_in(base_key, 2), -4.0, 4.0, (D, HD * KVH), jnp.float32) * D ** (-0.5)
    return (query_part, key_part)


def draw_w_query(key, part):
    query_part = weight_pair(key)[0]
    return query_part.astype(jnp.bfloat16)


def draw_w_key(key, part):
    query_part, key_part = weight_pair(key)
    return key_part.astype(jnp.bfloat16)


def draw_query_gain(key, part):
    sample_key = jax.random.fold_in(key, 31)
    return jax.random.uniform(sample_key, (HD,), jnp.float32, 0.6, 1.6)


def draw_key_gain(key, part):
    sample_key = jax.random.fold_in(key, 37)
    return jax.random.uniform(sample_key, (HD,), jnp.float32, 0.6, 1.6)


def bound_pair(key):
    base_key = jax.random.fold_in(key, 23)
    valid_counts = jax.random.randint(jax.random.fold_in(base_key, 1), (MICRO,), TOKENS // 2, TOKENS + 1, jnp.int32)
    full_pick = jax.random.randint(jax.random.fold_in(base_key, 3), (), 0, MICRO, jnp.int32)
    valid_counts = jnp.where(jnp.arange(MICRO, dtype=jnp.int32) == full_pick, TOKENS, valid_counts).astype(jnp.int32)
    back_steps = jax.random.randint(jax.random.fold_in(base_key, 2), (MICRO,), 0, TOK_DEV, jnp.int32)
    return (valid_counts, valid_counts - 1 - back_steps)


def draw_lengths(key, part):
    return bound_pair(key)[0]


def draw_reward_pos(key, part):
    return bound_pair(key)[1]


def steps_of(own_key, shape, cuts, least, top_value):
    loudness = 1.0
    for dim, parts in cuts:
        draws = jax.random.uniform(jax.random.fold_in(jax.random.fold_in(own_key, 6), dim), (parts,), jnp.float32, least / len(cuts), top_value / len(cuts))
        loudness = loudness * jnp.repeat(jnp.exp(draws), shape[dim] // parts).reshape((-1,) + (1,) * (len(shape) - 1 - dim))
    return loudness


def scatter_about(key, shape, deviation, bound, shards=(), kind=jnp.bfloat16):
    drawn = deviation * jax.random.normal(key, shape, jnp.float32)
    if shards:
        drawn = drawn * steps_of(key, shape, shards, -0.22, 0.18)
    return jnp.clip(drawn, -bound, bound).astype(kind)


def setup_inputs(seed: int = 0) -> dict:
    splits = jax.random.split(jax.random.key(seed), 14)
    return {
        "hidden": scatter_about(splits[0], (MICRO, TOKENS, D), 1.0, 6.0, ((1, 128),)),
        "lengths": draw_lengths(jax.random.fold_in(splits[13], 71), 0),
        "reward_pos": draw_reward_pos(jax.random.fold_in(splits[13], 71), 0),
        "in_gain": jnp.clip(1.0 + 0.18 * jax.random.normal(splits[3], (D,), jnp.float32), 0.099609375, 1.8984375).astype(jnp.bfloat16),
        "w_query": draw_w_query(jax.random.fold_in(splits[13], 71), 0),
        "w_key": draw_w_key(jax.random.fold_in(splits[13], 71), 0),
        "w_value": scatter_about(splits[6], (D, HD * KVH), D ** -0.5, 0.125, ((0, 128), (1, 4))),
        "query_gain": draw_query_gain(jax.random.fold_in(splits[13], 71), 0),
        "key_gain": draw_key_gain(jax.random.fold_in(splits[13], 71), 0),
        "w_out": scatter_about(splits[9], (GROUP * HD * KVH, D), (GROUP * HD * KVH) ** -0.5, 0.125, ((0, 4), (1, 128))),
        "post_gain": jnp.clip(1.0 + 0.18 * jax.random.normal(splits[10], (D,), jnp.float32), 0.099609375, 1.8984375).astype(jnp.bfloat16),
        "final_gain": jnp.clip(1.0 + 0.18 * jax.random.normal(splits[11], (D,), jnp.float32), 0.099609375, 1.8984375).astype(jnp.bfloat16),
        "value_head": scatter_about(splits[12], (D,), D ** -0.5, 0.125, ((0, 128),)),
    }


norm_eps = 1e-06
query_scale = 168.0 ** (-0.5)
rope_base = 10000.0

def rms_scale(values, gain_vec):
    return values * lax.rsqrt(lax.optimization_barrier(jnp.mean(values * values, axis=-1, keepdims=True)) + norm_eps) * gain_vec.astype(jnp.float32)

def rotate_pairs(head_rows, positions):
    half_width = head_rows.shape[-1] // 2
    frequency = rope_base ** (-jnp.arange(half_width, dtype=jnp.float32) * 2.0 / head_rows.shape[-1])
    angles = positions.astype(jnp.float32)[:, None] * frequency[None, :]
    target = (angles.shape[0],) + (1,) * (head_rows.ndim - 2) + (half_width,)
    cosine = jnp.cos(angles).reshape(target)
    sine_part = jnp.sin(angles).reshape(target)
    front_half = head_rows[..., :half_width]
    back_half = head_rows[..., half_width:]
    return jnp.concatenate([front_half * cosine - back_half * sine_part, back_half * cosine + front_half * sine_part], axis=-1)

def window_attention(queries, keys_all, values_all, query_pos, key_pos):
    scores = jnp.einsum('qhgd,khd->hgqk', queries.astype(jnp.float32), keys_all.astype(jnp.float32))
    allowed = (key_pos[None, :] <= query_pos[:, None]) & (key_pos[None, :] > query_pos[:, None] - WINDOW) & (key_pos[None, :] >= 0)
    scores = jnp.where(allowed[None, None], scores, -1e+30)
    row_top = lax.optimization_barrier(jnp.max(scores, axis=-1, keepdims=True))
    exponent = jnp.exp(scores - row_top)
    attn_weights = (exponent / lax.optimization_barrier(jnp.sum(exponent, axis=-1, keepdims=True))).astype(jnp.bfloat16)
    mixed_heads = jnp.einsum('hgqk,khd->qhgd', attn_weights.astype(jnp.float32), values_all.astype(jnp.float32))
    return mixed_heads.astype(jnp.bfloat16)

def apply_layer(residual, in_gain, w_query, w_key, w_value, query_gain, key_gain, w_out, post_gain):
    widened = residual.astype(jnp.float32)
    normed = rms_scale(widened, in_gain).astype(jnp.bfloat16)
    queries = jnp.dot(normed, w_query, preferred_element_type=jnp.float32).reshape(TOKENS, KVH, GROUP, HD)
    keys_new = jnp.dot(normed, w_key, preferred_element_type=jnp.float32).reshape(TOKENS, KVH, HD)
    vals_new = jnp.dot(normed, w_value, preferred_element_type=jnp.float32).reshape(TOKENS, KVH, HD)
    positions = jnp.arange(TOKENS, dtype=jnp.int32)
    queries = (rotate_pairs(rms_scale(queries, query_gain), positions) * query_scale).astype(jnp.bfloat16)
    keys_new = rotate_pairs(rms_scale(keys_new, key_gain), positions).astype(jnp.bfloat16)
    vals_new = vals_new.astype(jnp.bfloat16)
    pad_keys = jnp.concatenate([jnp.zeros((WINDOW, KVH, HD), jnp.bfloat16), keys_new], axis=0)
    pad_vals = jnp.concatenate([jnp.zeros((WINDOW, KVH, HD), jnp.bfloat16), vals_new], axis=0)

    def one_block(block_id):
        start_row = (block_id * TOK_DEV).astype(jnp.int32)
        block_queries = lax.dynamic_slice_in_dim(queries, start_row, TOK_DEV, 0)
        block_keys = lax.dynamic_slice_in_dim(pad_keys, start_row, WINDOW + TOK_DEV, 0)
        block_vals = lax.dynamic_slice_in_dim(pad_vals, start_row, WINDOW + TOK_DEV, 0)
        query_pos = start_row + jnp.arange(TOK_DEV, dtype=jnp.int32)
        key_pos = start_row - WINDOW + jnp.arange(WINDOW + TOK_DEV, dtype=jnp.int32)
        return window_attention(block_queries, block_keys, block_vals, query_pos, key_pos)
    mixed_heads = lax.map(one_block, jnp.arange(N_SEQ, dtype=jnp.int32)).reshape(TOKENS, GROUP * HD * KVH)
    branch = jnp.dot(mixed_heads, w_out, preferred_element_type=jnp.float32)
    return (widened + rms_scale(branch, post_gain)).astype(jnp.bfloat16)

def reference(hidden, lengths, reward_pos, in_gain, w_query, w_key, w_value, query_gain, key_gain, w_out, post_gain, final_gain, value_head):
    value_rows = []
    reward_rows = []
    positions = jnp.arange(TOKENS, dtype=jnp.int32)
    for micro_id in range(MICRO):
        residual = apply_layer(hidden[micro_id], in_gain, w_query, w_key, w_value, query_gain, key_gain, w_out, post_gain)
        last_rows = rms_scale(residual.astype(jnp.float32), final_gain).astype(jnp.bfloat16)
        raw_values = jnp.dot(last_rows, value_head, preferred_element_type=jnp.float32)
        raw_values = jnp.where(positions < lengths[micro_id], raw_values, 0.0)
        value_rows.append(raw_values)
        reward_rows.append(jnp.sum(jnp.where(positions == reward_pos[micro_id], raw_values, 0.0)))
    return (jnp.stack(value_rows), jnp.stack(reward_rows))
```

```python
import jax
import jax.numpy as jnp
import numpy as np
from jax import lax
from jax.experimental import pallas as pl
from jax.experimental.pallas import tpu as pltpu
from jax.sharding import Mesh
from jax.sharding import PartitionSpec as P

HD = 128
GROUP = 2
WINDOW = 1024
NORM_EPS = 1e-06
QUERY_SCALE = 168.0 ** (-0.5)
ROPE_BASE = 10000.0
SIZES = (2, 2, 8, 8, 2)
AXES = ("xh", "core", "z", "y", "xl")
SECTION = ("xh", "core")
SEQ = ("z", "y", "xl")
RING_X = ("xh", "xl")
NT = (((1,), (1,)), ((), ()))


def pairs_of(source_of):
    out = []
    for there in np.ndindex(*SIZES):
        here = source_of(*there)
        if here is not None:
            out.append(
                (int(np.ravel_multi_index(here, SIZES)), int(np.ravel_multi_index(there, SIZES)))
            )
    return out


def row_source(xh, c, z, y, l):
    return (xh, l, z, (8 * c + y) // 2, y % 2)


def out_source(xh, c, z, y, l):
    s, o = divmod(2 * z + c, 4)
    q = 32 * (2 * xh + l) + 8 * o + y
    return (s // 2, s % 2, q // 16, (q % 16) // 2, q % 2)


def other_half(xh, c, z, y, l):
    return (xh, c, z, y, 1 - l)


def block_before(xh, c, z, y, l):
    block = 8 * z + y - 1
    return None if block < 0 else (xh, c, block // 8, block % 8, l)


def moved(array, source_of):
    return lax.ppermute(array, AXES, pairs_of(source_of))


def told_to_all(array, axes):
    n = lax.axis_size(axes)
    return lax.all_to_all(jnp.broadcast_to(array[None], (n, *array.shape)), axes, 0, 0, tiled=True)


def project_kernel(first, h_ref, w_ref, gain_ref, cos_ref, sin_ref, out_ref, inv_ref):
    j = pl.program_id(0)

    @pl.when(j == 0)
    def _():
        wide = h_ref[...].astype(jnp.float32)
        inv_ref[...] = lax.rsqrt(jnp.mean(wide * wide, axis=1, keepdims=True) + NORM_EPS)

    acc = jnp.dot(h_ref[...], w_ref[...], preferred_element_type=jnp.float32) * inv_ref[...]

    @pl.when(j + first < 6)
    def _():
        unit = acc * lax.rsqrt(jnp.mean(acc * acc, axis=1, keepdims=True) + NORM_EPS)
        unit = unit * gain_ref[0]
        turned = pltpu.roll(unit, HD // 2, 1)
        out_ref[...] = (unit * cos_ref[...] + turned * sin_ref[...]).astype(jnp.bfloat16)

    @pl.when(j + first >= 6)
    def _():
        out_ref[...] = acc.astype(jnp.bfloat16)


def project(h, weights, gains, cos, sin, first):
    rows, width = h.shape
    whole = lambda *shape: pl.BlockSpec(shape, lambda j: (0,) * len(shape))
    return pl.pallas_call(
        lambda *refs: project_kernel(first, *refs),
        grid=(4,),
        in_specs=[
            whole(rows, width),
            pl.BlockSpec((width, HD), lambda j: (0, j + first)),
            pl.BlockSpec((1, 1, HD), lambda j: (j + first, 0, 0)),
            whole(rows, HD),
            whole(rows, HD),
        ],
        out_specs=pl.BlockSpec((rows, HD), lambda j: (0, j)),
        out_shape=jax.ShapeDtypeStruct((rows, 4 * HD), jnp.bfloat16),
        scratch_shapes=[pltpu.VMEM((rows, 1), jnp.float32)],
        name="project",
    )(h, weights, gains, cos, sin)


def attend_kernel(block_ref, q_ref, *refs):
    keys, vals, out_ref = refs[:5], refs[5:10], refs[10]
    rows = q_ref.shape[0]
    block = block_ref[0]
    query = lax.broadcasted_iota(jnp.int32, (rows, rows), 0)
    key = lax.broadcasted_iota(jnp.int32, (rows, rows), 1)
    for g in range(GROUP):
        q = q_ref[:, g * HD : (g + 1) * HD]
        scores = []
        for back in range(5):
            s = lax.dot_general(q, keys[back][...], NT, preferred_element_type=jnp.float32)
            if back == 0:
                s = jnp.where(key <= query, s, -1e30)
            elif back == 4:
                s = jnp.where((key > query) & (block >= 4), s, -1e30)
            else:
                s = jnp.where(block >= back, s, -1e30)
            scores.append(s)
        top = jnp.max(scores[0], axis=1, keepdims=True)
        for s in scores[1:]:
            top = jnp.maximum(top, jnp.max(s, axis=1, keepdims=True))
        total, mixed = 0.0, 0.0
        for s, v in zip(scores, vals):
            e = jnp.exp(s - top)
            total = total + jnp.sum(e, axis=1, keepdims=True)
            mixed = mixed + jnp.dot(
                e.astype(jnp.bfloat16), v[...], preferred_element_type=jnp.float32
            )
        out_ref[:, g * HD : (g + 1) * HD] = (mixed / total).astype(jnp.bfloat16)


def attend(block, q, held):
    rows = q.shape[0]
    part = lambda at: pl.BlockSpec((rows, HD), lambda h, b: (0, h + at))
    wide = pl.BlockSpec((rows, GROUP * HD), lambda h, b: (0, h))
    return pl.pallas_call(
        attend_kernel,
        grid_spec=pltpu.PrefetchScalarGridSpec(
            num_scalar_prefetch=1,
            grid=(2,),
            in_specs=[wide] + [part(0)] * 5 + [part(2)] * 5,
            out_specs=wide,
        ),
        out_shape=jax.ShapeDtypeStruct(q.shape, jnp.bfloat16),
        name="attend",
    )(block, q, *held, *held)


def sums_kernel(mixed_ref, w_ref, h_ref, out_ref):
    @pl.when(pl.program_id(0) == 0)
    def _():
        out_ref[...] = jnp.zeros_like(out_ref)

    width = mixed_ref.shape[2]
    branch = 0.0
    for s in range(4):
        branch = branch + lax.dot_general(
            w_ref[s, 0, :, :width], mixed_ref[s], NT, preferred_element_type=jnp.float32
        )
    gains = w_ref[0, 0, :, width:].astype(jnp.float32)
    post, final, head = gains[:, 0:1], gains[:, 1:2], gains[:, 2:3]
    read = final * head
    hidden = h_ref[0].astype(jnp.float32)
    scaled = branch * post
    for k, term in enumerate(
        (
            branch * branch,
            scaled * scaled,
            hidden * scaled,
            scaled * read,
            hidden * read,
            hidden * hidden,
        )
    ):
        out_ref[k : k + 1, :] += jnp.sum(term, axis=0, keepdims=True)


def token_sums(mixed, weights, h_share):
    rows = mixed.shape[1]
    _, parts, depth, wide = weights.shape
    return pl.pallas_call(
        sums_kernel,
        grid=(parts,),
        in_specs=[
            pl.BlockSpec(mixed.shape, lambda o: (0, 0, 0)),
            pl.BlockSpec((4, 1, depth, wide), lambda o: (0, o, 0, 0)),
            pl.BlockSpec((1, depth, rows), lambda o: (o, 0, 0)),
        ],
        out_specs=pl.BlockSpec((8, rows), lambda o: (0, 0)),
        out_shape=jax.ShapeDtypeStruct((8, rows), jnp.float32),
        name="token_sums",
    )(mixed, weights, h_share)


def local(
    hidden,
    lengths,
    reward_pos,
    in_gain,
    w_query,
    w_key,
    w_value,
    query_gain,
    key_gain,
    w_out,
    post_gain,
    final_gain,
    value_head,
):
    _, tok_dev, width = hidden.shape
    shard = in_gain.shape[0]
    rows = 2 * tok_dev
    block = 8 * lax.axis_index("z") + lax.axis_index("y")
    core, half = lax.axis_index("core"), lax.axis_index("xl")
    place = 2 * lax.axis_index("xh") + half

    projections = jnp.concatenate([w_query, w_key, w_value], axis=1).astype(jnp.float32)
    projections = (projections * in_gain.astype(jnp.float32)[:, None]).astype(jnp.bfloat16)
    octet = told_to_all(moved(projections, row_source), "y").reshape(8 * shard, -1)
    weights = lax.all_gather(octet, ("z", "core"), axis=0, tiled=True)

    extra = jnp.stack([post_gain, final_gain, value_head], axis=1)
    out_shard = jnp.concatenate(
        [w_out.T, extra, jnp.zeros((shard, HD - 3), jnp.bfloat16)], axis=1
    )
    out_octet = told_to_all(moved(out_shard, out_source), "y").reshape(8 * shard, -1)
    out_weights = lax.all_gather(out_octet, ("z", "core"), axis=0, tiled=True)
    out_weights = out_weights.reshape(4, 4, 8 * shard, -1)

    mine = lax.dynamic_index_in_dim(hidden, core, 0, keepdims=False)
    theirs = moved(mine, other_half)
    h = jnp.concatenate(
        [jnp.where(half == 0, mine, theirs), jnp.where(half == 0, theirs, mine)], axis=0
    )
    h_share = lax.dynamic_slice_in_dim(h, place * (width // 4), width // 4, 1)
    h_share = h_share.T.reshape(4, 8 * shard, rows)

    pos = block * rows + jnp.arange(rows, dtype=jnp.int32)
    frequency = ROPE_BASE ** (-jnp.arange(HD // 2, dtype=jnp.float32) * 2.0 / HD)
    angles = pos.astype(jnp.float32)[:, None] * frequency[None, :]
    cos, sin = jnp.cos(angles), jnp.sin(angles)
    cos = jnp.concatenate([cos, cos], axis=1)
    sin = jnp.concatenate([-sin, sin], axis=1)
    gains = jnp.stack([query_gain * QUERY_SCALE] * 4 + [key_gain] * 4)[:, None, :]

    kv = project(h, weights, gains, cos, sin, 4)
    held = [kv]
    for _ in range(WINDOW // rows):
        held.append(moved(held[-1], block_before))
    q = project(h, weights, gains, cos, sin, 0)
    mixed = attend(block[None], q, held)

    everyone = told_to_all(mixed, RING_X)
    sums = token_sums(everyone, out_weights, h_share)
    sums = told_to_all(sums, ("xh", "xl", "core")).reshape(4, 2, 8, rows).sum(axis=0)
    branch_sq, scaled_sq, cross, read_branch, read_hidden, hidden_sq = (
        sums[:, k] for k in range(6)
    )
    scale = lax.rsqrt(branch_sq / width + NORM_EPS)
    residual_sq = hidden_sq + scale * (2.0 * cross + scale * scaled_sq)
    residual_sq = jnp.maximum(residual_sq, 0.0)
    values = (read_hidden + scale * read_branch) * lax.rsqrt(residual_sq / width + NORM_EPS)
    values = jnp.where(pos[None, :] < lengths[:, None], values, 0.0)
    token_values = lax.dynamic_slice_in_dim(values, half * tok_dev, tok_dev, 1)
    reward = jnp.sum(jnp.where(pos[None, :] == reward_pos[:, None], values, 0.0), axis=1)
    for axis in ("y", "z"):
        reward = told_to_all(reward, axis).sum(axis=0)
    return token_values, reward


def solution(mesh):
    torus = Mesh(mesh.devices.reshape(SIZES), AXES)
    in_specs = (
        P(None, SEQ, None),
        P(),
        P(),
        P(SEQ),
        P(SEQ, SECTION),
        P(SEQ, SECTION),
        P(SEQ, SECTION),
        P(),
        P(),
        P(SECTION, SEQ),
        P(SEQ),
        P(SEQ),
        P(SEQ),
    )
    out_specs = (P(None, SEQ), P())
    return jax.shard_map(local, mesh=torus, in_specs=in_specs, out_specs=out_specs, check_vma=False)
```

```python
import jax
import jax.numpy as jnp
import numpy as np
from jax import lax
from jax.experimental import pallas as pl
from jax.experimental.pallas import tpu as pltpu
from jax.sharding import Mesh
from jax.sharding import PartitionSpec as P


HD = 128
GROUP = 2
NORM_EPS = 1e-06
QUERY_SCALE = 168.0 ** (-0.5)
ROPE_BASE = 10000.0
SIZES = (2, 2, 8, 4, 2, 2)
AXES = ("xh", "core", "z", "yy", "p", "xl")
SECTION = ("xh", "core")
SEQ = ("z", "yy", "p", "xl")
AXIS_Y = ("yy", "p")
OCTANT = ("xh", "xl", "p")
NT = (((1,), (1,)), ((), ()))


def pairs_of(source_of):
    out = []
    for there in np.ndindex(*SIZES):
        here = source_of(*there)
        if here is not None:
            out.append(
                (int(np.ravel_multi_index(here, SIZES)), int(np.ravel_multi_index(there, SIZES)))
            )
    return out


def row_source(xh, c, z, yy, p, l):
    return (xh, l, z, 2 * c + yy // 2, yy % 2, p)


def out_source(xh, c, z, yy, p, l):
    s, o = divmod(2 * z + c, 4)
    q = 32 * (2 * xh + l) + 8 * o + 2 * yy + p
    return (s // 2, s % 2, q // 16, (q // 4) % 4, (q // 2) % 2, q % 2)


def beside(across_p, across_l):
    return lambda xh, c, z, yy, p, l: (xh, c, z, yy, p ^ across_p, l ^ across_l)


def block_before(xh, c, z, yy, p, l):
    block = 4 * z + yy - 1
    return None if block < 0 else (xh, c, block // 4, block % 4, p, l)


def moved(array, source_of):
    return lax.ppermute(array, AXES, pairs_of(source_of))


def told_to_all(array, axes):
    n = lax.axis_size(axes)
    return lax.all_to_all(jnp.broadcast_to(array[None], (n, *array.shape)), axes, 0, 0, tiled=True)


def exchanged(tiles, axes):
    return lax.all_to_all(tiles, axes, 0, 0, tiled=True)


def norm_kernel(order_ref, gain_ref, *refs):
    for k in range(4):
        wide = refs[k][...].astype(jnp.float32)
        inverse = lax.rsqrt(jnp.mean(wide * wide, axis=1, keepdims=True) + NORM_EPS)
        rows = wide.shape[0]
        at = pl.multiple_of(order_ref[k] * rows, rows)
        refs[4][pl.ds(at, rows), :] = (wide * inverse * gain_ref[...]).astype(jnp.bfloat16)


def normed_rows(order, gain, pieces):
    rows, width = pieces[0].shape
    vmem = pl.BlockSpec(memory_space=pltpu.VMEM)
    return pl.pallas_call(
        norm_kernel,
        in_specs=[pl.BlockSpec(memory_space=pltpu.SMEM)] + [vmem] * 5,
        out_specs=vmem,
        out_shape=jax.ShapeDtypeStruct((4 * rows, width), jnp.bfloat16),
        name="norm",
    )(order, gain, *pieces)


def project_kernel(turned_heads, rows_ref, w_ref, gain_ref, cos_ref, sin_ref, out_ref):
    acc = jnp.dot(rows_ref[...], w_ref[...], preferred_element_type=jnp.float32)

    def turn():
        unit = acc * lax.rsqrt(jnp.mean(acc * acc, axis=1, keepdims=True) + NORM_EPS)
        unit = unit * gain_ref[...]
        other = pltpu.roll(unit, HD // 2, 1)
        out_ref[...] = (unit * cos_ref[...] + other * sin_ref[...]).astype(jnp.bfloat16)

    if turned_heads == 2:
        turn()
    else:
        pl.when(pl.program_id(0) == 0)(turn)

        @pl.when(pl.program_id(0) == 1)
        def _():
            out_ref[...] = acc.astype(jnp.bfloat16)


def project(normed, weights, gain, cos, sin, first, turned_heads):
    rows, width = normed.shape
    vmem = pl.BlockSpec(memory_space=pltpu.VMEM)
    return pl.pallas_call(
        lambda *refs: project_kernel(turned_heads, *refs),
        grid=(2,),
        in_specs=[
            vmem,
            pl.BlockSpec((width, HD), lambda j: (0, j + first)),
            vmem,
            vmem,
            vmem,
        ],
        out_specs=pl.BlockSpec((rows, HD), lambda j: (0, j)),
        out_shape=jax.ShapeDtypeStruct((rows, 2 * HD), jnp.bfloat16),
        name="project",
    )(normed, weights, gain, cos, sin)


def attend_kernel(block_ref, q_ref, own_ref, back1_ref, back2_ref, out_ref):
    held = (back2_ref, back1_ref, own_ref)
    rows = q_ref.shape[0] // 2
    block = block_ref[0]
    query = lax.broadcasted_iota(jnp.int32, (rows, rows), 0)
    key = lax.broadcasted_iota(jnp.int32, (rows, rows), 1)
    for a in range(2):
        pieces = [
            held[i // 2][(i % 2) * rows : (i % 2 + 1) * rows, :] for i in range(a, a + 5)
        ]
        for g in range(GROUP):
            q = q_ref[a * rows : (a + 1) * rows, g * HD : (g + 1) * HD]
            scores = []
            for k, piece in enumerate(pieces):
                s = lax.dot_general(q, piece[:, :HD], NT, preferred_element_type=jnp.float32)
                there = 2 * block + (a + k - 4) >= 0
                if k == 4:
                    s = jnp.where(key <= query, s, -1e30)
                elif k == 0:
                    s = jnp.where((key > query) & there, s, -1e30)
                elif a + k < 4:
                    s = jnp.where(there, s, -1e30)
                scores.append(s)
            top = jnp.max(scores[0], axis=1, keepdims=True)
            for s in scores[1:]:
                top = jnp.maximum(top, jnp.max(s, axis=1, keepdims=True))
            total, mixed = 0.0, 0.0
            for s, piece in zip(scores, pieces):
                e = jnp.exp(s - top)
                total = total + jnp.sum(e, axis=1, keepdims=True)
                mixed = mixed + jnp.dot(
                    e.astype(jnp.bfloat16), piece[:, HD:], preferred_element_type=jnp.float32
                )
            mixed = (mixed / total).astype(jnp.bfloat16)
            for x in range(4):
                out_ref[2 * x + a, :, g * HD : (g + 1) * HD] = mixed


def attend(block, q, held):
    rows, wide = q.shape
    vmem = pl.BlockSpec(memory_space=pltpu.VMEM)
    return pl.pallas_call(
        attend_kernel,
        in_specs=[pl.BlockSpec(memory_space=pltpu.SMEM)] + [vmem] * 4,
        out_specs=vmem,
        out_shape=jax.ShapeDtypeStruct((8, rows // 2, wide), jnp.bfloat16),
        name="attend",
    )(block, q, *held)


def sums_kernel(mixed_ref, w_ref, gains_ref, h_ref, out_ref, sums_ref):
    o = pl.program_id(0)

    @pl.when(o == 0)
    def _():
        sums_ref[...] = jnp.zeros_like(sums_ref)

    wide = mixed_ref.shape[2]
    branch = 0.0
    for head in range(8):
        at = (head % 2) * wide
        branch = branch + lax.dot_general(
            w_ref[head // 2, 0, :, at : at + wide],
            mixed_ref[head],
            NT,
            preferred_element_type=jnp.float32,
        )
    gains = gains_ref[0]
    post, final, head = gains[:, 0:1], gains[:, 1:2], gains[:, 2:3]
    read = final * head
    hidden = h_ref[0].astype(jnp.float32)
    scaled = branch * post
    for k, term in enumerate(
        (
            branch * branch,
            scaled * scaled,
            hidden * scaled,
            scaled * read,
            hidden * read,
            hidden * hidden,
        )
    ):
        sums_ref[k : k + 1, :] += jnp.sum(term, axis=0, keepdims=True)

    @pl.when(o == pl.num_programs(0) - 1)
    def _():
        for k in range(out_ref.shape[0]):
            out_ref[k] = sums_ref[...]


def token_sums(mixed, weights, gains, h_share, copies):
    rows = mixed.shape[1]
    _, parts, depth, wide = weights.shape
    return pl.pallas_call(
        sums_kernel,
        grid=(parts,),
        in_specs=[
            pl.BlockSpec(memory_space=pltpu.VMEM),
            pl.BlockSpec((4, 1, depth, wide), lambda o: (0, o, 0, 0)),
            pl.BlockSpec((1, depth, 3), lambda o: (o, 0, 0)),
            pl.BlockSpec((1, depth, rows), lambda o: (o, 0, 0)),
        ],
        out_specs=pl.BlockSpec((copies, 8, rows), lambda o: (0, 0, 0)),
        out_shape=jax.ShapeDtypeStruct((copies, 8, rows), jnp.float32),
        scratch_shapes=[pltpu.VMEM((8, rows), jnp.float32)],
        name="token_sums",
    )(mixed, weights, gains, h_share)


def local(
    hidden,
    lengths,
    reward_pos,
    in_gain,
    w_query,
    w_key,
    w_value,
    query_gain,
    key_gain,
    w_out,
    post_gain,
    final_gain,
    value_head,
):
    _, tok_dev, width = hidden.shape
    shard = in_gain.shape[0]
    octet_rows = 8 * shard
    rows = 2 * tok_dev
    block = 4 * lax.axis_index("z") + lax.axis_index("yy")
    parity, half = lax.axis_index("p"), lax.axis_index("xl")
    place = 2 * lax.axis_index("xh") + half

    def with_row(tile, values):
        return jnp.concatenate([tile, jnp.pad(values, (0, 4 * HD - values.shape[0]))[None]], axis=0)

    heads = [
        with_row(
            jnp.concatenate(
                [
                    w_query[:, 2 * k * HD : 2 * (k + 1) * HD],
                    w_key[:, k * HD : (k + 1) * HD],
                    w_value[:, k * HD : (k + 1) * HD],
                ],
                axis=1,
            ),
            in_gain,
        )
        for k in range(2)
    ]
    out_shard = with_row(w_out.T, jnp.concatenate([post_gain, final_gain, value_head]))
    heads = moved(jnp.stack(heads), row_source)
    out_shard = moved(out_shard, out_source)
    tiles = jnp.concatenate(
        [jnp.tile(heads, (4, 1, 1)), jnp.broadcast_to(out_shard, (8, *out_shard.shape))], axis=2
    )
    octet = exchanged(tiles, AXIS_Y)
    gains = [octet[:, shard, at : at + shard] for at in (0, *range(4 * HD, 4 * HD + 3 * shard, shard))]
    gains = jnp.stack(gains).reshape(4, octet_rows)
    gains = jnp.pad(gains, ((0, 0), (0, 256 - octet_rows)))
    octet = octet[:, :shard].reshape(octet_rows, 8 * HD)
    weights = lax.all_gather(octet[:, : 4 * HD], ("z", "core"), axis=0, tiled=True)
    out_weights = lax.all_gather(octet[:, 4 * HD :], ("z", "core"), axis=0, tiled=True)
    out_weights = out_weights.reshape(4, 4, octet_rows, -1)
    gains = told_to_all(gains, ("z", "core"))
    gains = gains[:, :, :octet_rows].astype(jnp.float32)
    in_full = gains[:, 0].reshape(1, width)
    out_gains = gains[:4, 1:].swapaxes(1, 2)

    mine = lax.dynamic_index_in_dim(hidden, lax.axis_index("core"), 0, keepdims=False)
    near = moved(mine, beside(0, 1))
    far = moved(mine, beside(1, 0)), moved(mine, beside(1, 1))
    pieces = (mine, near, *far)
    order = jnp.stack(
        [
            2 * parity + half,
            2 * parity + 1 - half,
            2 - 2 * parity + half,
            2 - 2 * parity + 1 - half,
        ]
    )
    normed = normed_rows(order, in_full, pieces)
    h_share = jnp.concatenate(
        [jnp.where(half == 0, mine, near), jnp.where(half == 0, near, mine)], axis=0
    )
    h_share = lax.dynamic_slice_in_dim(h_share, place * (width // 4), width // 4, 1)
    h_share = h_share.T.reshape(4, octet_rows, rows)

    pos = block * 2 * rows + jnp.arange(2 * rows, dtype=jnp.int32)
    frequency = ROPE_BASE ** (-jnp.arange(HD // 2, dtype=jnp.float32) * 2.0 / HD)
    angles = pos.astype(jnp.float32)[:, None] * frequency[None, :]
    cos, sin = jnp.cos(angles), jnp.sin(angles)
    cos = jnp.concatenate([cos, cos], axis=1)
    sin = jnp.concatenate([-sin, sin], axis=1)

    held = [project(normed, weights, key_gain[None], cos, sin, 2, 1)]
    for _ in range(2):
        held.append(moved(held[-1], block_before))
    q = project(normed, weights, (query_gain * QUERY_SCALE)[None], cos, sin, 0, 2)
    mixed = exchanged(attend(block[None], q, held), OCTANT)

    sums = exchanged(token_sums(mixed, out_weights, out_gains, h_share, 16), OCTANT + ("core",))
    sums = sums.reshape(4, 2, 2, 8, rows).sum(axis=0)
    branch_sq, scaled_sq, cross, read_branch, read_hidden, hidden_sq = (
        sums[:, :, k] for k in range(6)
    )
    scale = lax.rsqrt(branch_sq / width + NORM_EPS)
    residual_sq = hidden_sq + scale * (2.0 * cross + scale * scaled_sq)
    residual_sq = jnp.maximum(residual_sq, 0.0)
    values = (read_hidden + scale * read_branch) * lax.rsqrt(residual_sq / width + NORM_EPS)
    pos = pos.reshape(2, 1, rows)
    values = jnp.where(pos < lengths[None, :, None], values, 0.0)
    reward = jnp.sum(jnp.where(pos == reward_pos[None, :, None], values, 0.0), axis=(0, 2))
    reward = told_to_all(reward, ("z", "yy")).sum(axis=0)
    token_values = lax.dynamic_index_in_dim(values, parity, 0, keepdims=False)
    token_values = lax.dynamic_slice_in_dim(token_values, half * tok_dev, tok_dev, 1)
    return token_values, reward


def solution(mesh):
    torus = Mesh(mesh.devices.reshape(SIZES), AXES)
    in_specs = (
        P(None, SEQ, None),
        P(),
        P(),
        P(SEQ),
        P(SEQ, SECTION),
        P(SEQ, SECTION),
        P(SEQ, SECTION),
        P(),
        P(),
        P(SECTION, SEQ),
        P(SEQ),
        P(SEQ),
        P(SEQ),
    )
    out_specs = (P(None, SEQ), P())

    return jax.shard_map(local, mesh=torus, in_specs=in_specs, out_specs=out_specs, check_vma=False)
```

```python
import jax
import jax.numpy as jnp
import numpy as np
from jax import lax
from jax.experimental import pallas as pl
from jax.experimental.pallas import tpu as pltpu
from jax.sharding import Mesh
from jax.sharding import PartitionSpec as P


HD = 128
GROUP = 2
NORM_EPS = 1e-06
QUERY_SCALE = 168.0 ** (-0.5)
ROPE_BASE = 10000.0
SIZES = (2, 2, 8, 4, 2, 2)
AXES = ("xh", "core", "z", "yy", "p", "xl")
SECTION = ("xh", "core")
SEQ = ("z", "yy", "p", "xl")
AXIS_Y = ("yy", "p")
OCTANT = ("xh", "xl", "p")
NT = (((1,), (1,)), ((), ()))


def pairs_of(source_of):
    out = []
    for there in np.ndindex(*SIZES):
        here = source_of(*there)
        if here is not None:
            out.append(
                (int(np.ravel_multi_index(here, SIZES)), int(np.ravel_multi_index(there, SIZES)))
            )
    return out


def row_source(xh, c, z, yy, p, l):
    return (xh, l, z, 2 * c + yy // 2, yy % 2, p)


def out_source(xh, c, z, yy, p, l):
    s, o = divmod(2 * z + c, 4)
    q = 32 * (2 * xh + l) + 8 * o + 2 * yy + p
    return (s // 2, s % 2, q // 16, (q // 4) % 4, (q // 2) % 2, q % 2)


def beside(across_p, across_l):
    return lambda xh, c, z, yy, p, l: (xh, c, z, yy, p ^ across_p, l ^ across_l)


def block_before(xh, c, z, yy, p, l):
    block = 4 * z + yy - 1
    return None if block < 0 else (xh, c, block // 4, block % 4, p, l)


def moved(array, source_of):
    return lax.ppermute(array, AXES, pairs_of(source_of))


def told_to_all(array, axes):
    n = lax.axis_size(axes)
    return lax.all_to_all(jnp.broadcast_to(array[None], (n, *array.shape)), axes, 0, 0, tiled=True)


def exchanged(tiles, axes):
    return lax.all_to_all(tiles, axes, 0, 0, tiled=True)


def rms_rows(piece, gain):
    wide = piece.astype(jnp.float32)
    inverse = lax.rsqrt(jnp.mean(wide * wide, axis=1, keepdims=True) + NORM_EPS)
    return (wide * inverse * gain).astype(jnp.bfloat16)


def norm_kernel(order_ref, gain_ref, *refs):
    out_ref = refs[3]
    for k in range(4):
        rows = refs[0].shape[0]
        at = pl.multiple_of(order_ref[k] * rows, rows)
        if k < 3:
            out_ref[pl.ds(at, rows), :] = rms_rows(refs[k][...], gain_ref[...])
        else:
            out_ref[pl.ds(at, rows), :] = jnp.zeros((rows, out_ref.shape[1]), jnp.bfloat16)


def normed_rows(order, gain, pieces):
    rows, width = pieces[0].shape
    vmem = pl.BlockSpec(memory_space=pltpu.VMEM)
    return pl.pallas_call(
        norm_kernel,
        in_specs=[pl.BlockSpec(memory_space=pltpu.SMEM)] + [vmem] * 4,
        out_specs=vmem,
        out_shape=jax.ShapeDtypeStruct((4 * rows, width), jnp.bfloat16),
        name="norm",
    )(order, gain, *pieces)


def project_kernel(turns, order_ref, rows_ref, last_ref, in_gain_ref, w_ref, *refs):
    gain_ref, cos_ref, sin_ref = refs[:3]
    outs, normed_ref = refs[3:-1], refs[-1]
    j = pl.program_id(0)
    rows = last_ref.shape[0]
    at = pl.multiple_of(order_ref[3] * rows, rows)

    @pl.when(j == 0)
    def _():
        normed_ref[...] = rms_rows(last_ref[...], in_gain_ref[...])

    acc = jnp.dot(rows_ref[...], w_ref[...], preferred_element_type=jnp.float32)
    last = jnp.dot(normed_ref[...], w_ref[...], preferred_element_type=jnp.float32)

    def turned(tile, cos, sin):
        unit = tile * lax.rsqrt(jnp.mean(tile * tile, axis=1, keepdims=True) + NORM_EPS)
        unit = unit * gain_ref[...]
        return unit * cos + pltpu.roll(unit, HD // 2, 1) * sin

    def store(out_ref, turn):
        if turn:
            out_ref[...] = turned(acc, cos_ref[...], sin_ref[...]).astype(jnp.bfloat16)
            there = turned(last, cos_ref[pl.ds(at, rows), :], sin_ref[pl.ds(at, rows), :])
        else:
            out_ref[...] = acc.astype(jnp.bfloat16)
            there = last
        out_ref[pl.ds(at, rows), :] = there.astype(jnp.bfloat16)

    if len(outs) == 1:
        store(outs[0], True)
    else:
        for k in range(2):
            pl.when(j == k)(lambda k=k: store(outs[k], turns[k]))


def project(order, normed, last, in_gain, weights, gain, cos, sin, first, turns):
    rows, width = normed.shape
    vmem = pl.BlockSpec(memory_space=pltpu.VMEM)
    if turns[1]:
        out_specs = [pl.BlockSpec((rows, HD), lambda j: (0, j))]
        out_shape = [jax.ShapeDtypeStruct((rows, 2 * HD), jnp.bfloat16)]
    else:
        out_specs = [pl.BlockSpec((rows, HD), lambda j: (0, 0))] * 2
        out_shape = [jax.ShapeDtypeStruct((rows, HD), jnp.bfloat16)] * 2
    return pl.pallas_call(
        lambda *refs: project_kernel(turns, *refs),
        grid=(2,),
        in_specs=[
            pl.BlockSpec(memory_space=pltpu.SMEM),
            vmem,
            vmem,
            vmem,
            pl.BlockSpec((width, HD), lambda j: (0, j + first)),
            vmem,
            vmem,
            vmem,
        ],
        out_specs=out_specs,
        out_shape=out_shape,
        scratch_shapes=[pltpu.VMEM(last.shape, jnp.bfloat16)],
        name="project",
    )(order, normed, last, in_gain, weights, gain, cos, sin)


def part_of(ref, i, rows):
    return ref[i * rows : (i + 1) * rows, :]


def scores_of(q, k, place, block, query, key):
    s = lax.dot_general(q, k, NT, preferred_element_type=jnp.float32)
    a, i = place
    if i - a == 4:
        return jnp.where(key <= query, s, -1e30)
    if i >= 4:
        return s
    there = 2 * block + (i - 4) >= 0
    if i == a:
        return jnp.where((key > query) & there, s, -1e30)
    return jnp.where(there, s, -1e30)


def row_max(scores):
    top = jnp.max(scores[0], axis=1, keepdims=True)
    for s in scores[1:]:
        top = jnp.maximum(top, jnp.max(s, axis=1, keepdims=True))
    return top


def attend_kernel(block_ref, q_ref, *refs):
    keys, vals, out_ref = refs[2::-1], refs[5:2:-1], refs[6]
    rows = q_ref.shape[0] // 2
    query = lax.broadcasted_iota(jnp.int32, (rows, rows), 0)
    key = lax.broadcasted_iota(jnp.int32, (rows, rows), 1)
    for a in range(2):
        at = slice(a * rows, (a + 1) * rows)
        pieces = range(a, a + 5)
        for g in range(GROUP):
            wide = slice(g * HD, (g + 1) * HD)
            q = q_ref[at, wide]
            scores = [
                scores_of(q, part_of(keys[i // 2], i % 2, rows), (a, i), block_ref[0], query, key)
                for i in pieces
            ]
            top = row_max(scores)
            terms = [jnp.exp(s - top) for s in scores]
            total = sum(jnp.sum(e, axis=1, keepdims=True) for e in terms)
            share = 1.0 / total
            mixed = sum(
                jnp.dot(
                    (e * share).astype(jnp.bfloat16),
                    part_of(vals[i // 2], i % 2, rows),
                    preferred_element_type=jnp.float32,
                )
                for e, i in zip(terms, pieces)
            ).astype(jnp.bfloat16)
            for x in range(4):
                out_ref[2 * x + a, :, wide] = mixed


def attend(block, q, keys, vals):
    rows, wide = q.shape
    vmem = pl.BlockSpec(memory_space=pltpu.VMEM)
    return pl.pallas_call(
        attend_kernel,
        in_specs=[pl.BlockSpec(memory_space=pltpu.SMEM)] + [vmem] * 7,
        out_specs=vmem,
        out_shape=jax.ShapeDtypeStruct((8, rows // 2, wide), jnp.bfloat16),
        name="attend",
    )(block, q, *keys, *vals)


def sums_kernel(mixed_ref, w_ref, gains_ref, h_ref, branch_ref, out_ref, sums_ref):
    o = pl.program_id(0)

    @pl.when(o == 0)
    def _():
        sums_ref[...] = jnp.zeros_like(sums_ref)

    wide = mixed_ref.shape[2]
    branch = 0.0
    for head in range(8):
        at = (head % 2) * wide
        branch = branch + lax.dot_general(
            w_ref[head // 2, 0, :, at : at + wide],
            mixed_ref[head],
            NT,
            preferred_element_type=jnp.float32,
        )
    branch_ref[0] = branch
    hidden = h_ref[0].astype(jnp.float32)
    scaled = branch * gains_ref[0, :, 0:1]
    for k, term in enumerate((branch * branch, scaled * scaled, hidden * scaled, hidden * hidden)):
        sums_ref[k : k + 1, :] += jnp.sum(term, axis=0, keepdims=True)

    @pl.when(o == pl.num_programs(0) - 1)
    def _():
        for k in range(out_ref.shape[0]):
            out_ref[k] = sums_ref[...]


def token_sums(mixed, weights, gains, h_share, copies):
    rows = mixed.shape[1]
    _, parts, depth, wide = weights.shape
    return pl.pallas_call(
        sums_kernel,
        grid=(parts,),
        in_specs=[
            pl.BlockSpec(memory_space=pltpu.VMEM),
            pl.BlockSpec((4, 1, depth, wide), lambda o: (0, o, 0, 0)),
            pl.BlockSpec((1, depth, 3), lambda o: (o, 0, 0)),
            pl.BlockSpec((1, depth, rows), lambda o: (o, 0, 0)),
        ],
        out_specs=[
            pl.BlockSpec((1, depth, rows), lambda o: (o, 0, 0)),
            pl.BlockSpec((copies, 8, rows), lambda o: (0, 0, 0)),
        ],
        out_shape=[
            jax.ShapeDtypeStruct((parts, depth, rows), jnp.float32),
            jax.ShapeDtypeStruct((copies, 8, rows), jnp.float32),
        ],
        scratch_shapes=[pltpu.VMEM((8, rows), jnp.float32)],
        name="token_sums",
    )(mixed, weights, gains, h_share)


def values_kernel(sums_ref, branch_ref, gains_ref, h_ref, out_ref):
    sums = sum(sums_ref[x] for x in range(sums_ref.shape[0]))
    branch_sq, scaled_sq, cross, hidden_sq = (sums[k : k + 1] for k in range(4))
    parts, depth, _ = h_ref.shape
    width = 4 * parts * depth
    scale = lax.rsqrt(branch_sq / width + NORM_EPS)
    residual_sq = hidden_sq + scale * (2.0 * cross + scale * scaled_sq)
    last_scale = lax.rsqrt(jnp.maximum(residual_sq, 0.0) / width + NORM_EPS)
    value = 0.0
    for o in range(parts):
        post, final, head = (gains_ref[o, :, k : k + 1] for k in range(3))
        residual = h_ref[o].astype(jnp.float32) + branch_ref[o] * scale * post
        residual = residual.astype(jnp.bfloat16).astype(jnp.float32)
        last = (residual * last_scale * final).astype(jnp.bfloat16).astype(jnp.float32)
        value = value + jnp.sum(last * head, axis=0, keepdims=True)
    for k in range(out_ref.shape[0]):
        out_ref[k] = value


def partial_values(sums, branch, gains, h_share, copies):
    vmem = pl.BlockSpec(memory_space=pltpu.VMEM)
    return pl.pallas_call(
        values_kernel,
        in_specs=[vmem] * 4,
        out_specs=vmem,
        out_shape=jax.ShapeDtypeStruct((copies, 1, h_share.shape[2]), jnp.float32),
        name="partial_values",
    )(sums, branch, gains, h_share)


def local(
    hidden,
    lengths,
    reward_pos,
    in_gain,
    w_query,
    w_key,
    w_value,
    query_gain,
    key_gain,
    w_out,
    post_gain,
    final_gain,
    value_head,
):
    _, tok_dev, width = hidden.shape
    shard = in_gain.shape[0]
    octet_rows = 8 * shard
    rows = 2 * tok_dev
    block = 4 * lax.axis_index("z") + lax.axis_index("yy")
    parity, half = lax.axis_index("p"), lax.axis_index("xl")
    place = 2 * lax.axis_index("xh") + half

    def with_row(tile, values):
        return jnp.concatenate([tile, jnp.pad(values, (0, 4 * HD - values.shape[0]))[None]], axis=0)

    heads = [
        with_row(
            jnp.concatenate(
                [
                    w_query[:, 2 * k * HD : 2 * (k + 1) * HD],
                    w_key[:, k * HD : (k + 1) * HD],
                    w_value[:, k * HD : (k + 1) * HD],
                ],
                axis=1,
            ),
            in_gain,
        )
        for k in range(2)
    ]
    out_shard = with_row(w_out.T, jnp.concatenate([post_gain, final_gain, value_head]))
    heads = moved(jnp.stack(heads), row_source)
    out_shard = moved(out_shard, out_source)
    tiles = jnp.concatenate(
        [jnp.tile(heads, (4, 1, 1)), jnp.broadcast_to(out_shard, (8, *out_shard.shape))], axis=2
    )
    octet = exchanged(tiles, AXIS_Y)
    gains = [octet[:, shard, at : at + shard] for at in (0, *range(4 * HD, 4 * HD + 3 * shard, shard))]
    gains = jnp.stack(gains).reshape(4, octet_rows)
    gains = jnp.pad(gains, ((0, 0), (0, 256 - octet_rows)))
    octet = octet[:, :shard].reshape(octet_rows, 8 * HD)
    weights = lax.all_gather(octet[:, : 4 * HD], ("z", "core"), axis=0, tiled=True)
    out_weights = lax.all_gather(octet[:, 4 * HD :], ("z", "core"), axis=0, tiled=True)
    out_weights = out_weights.reshape(4, 4, octet_rows, -1)
    gains = told_to_all(gains, ("z", "core"))
    gains = gains[:, :, :octet_rows].astype(jnp.float32)
    in_full = gains[:, 0].reshape(1, width)
    out_gains = gains[:4, 1:].swapaxes(1, 2)

    mine = lax.dynamic_index_in_dim(hidden, lax.axis_index("core"), 0, keepdims=False)
    near = moved(mine, beside(0, 1))
    far = [moved(mine, beside(1, 0))]
    far.append(moved(mine, beside(1, 1)))
    pieces = (mine, near, *far)
    order = jnp.stack(
        [
            2 * parity + half,
            2 * parity + 1 - half,
            2 - 2 * parity + half,
            2 - 2 * parity + 1 - half,
        ]
    )
    normed = normed_rows(order, in_full, pieces[:3])
    h_share = jnp.concatenate(
        [jnp.where(half == 0, mine, near), jnp.where(half == 0, near, mine)], axis=0
    )
    h_share = lax.dynamic_slice_in_dim(h_share, place * (width // 4), width // 4, 1)
    h_share = h_share.T.reshape(4, octet_rows, rows)

    pos = block * 2 * rows + jnp.arange(2 * rows, dtype=jnp.int32)
    frequency = ROPE_BASE ** (-jnp.arange(HD // 2, dtype=jnp.float32) * 2.0 / HD)
    angles = pos.astype(jnp.float32)[:, None] * frequency[None, :]
    cos, sin = jnp.cos(angles), jnp.sin(angles)
    cos = jnp.concatenate([cos, cos], axis=1)
    sin = jnp.concatenate([-sin, sin], axis=1)

    shared = (order, normed, pieces[3], in_full, weights)
    key, val = project(*shared, key_gain[None], cos, sin, 2, (True, False))
    keys, vals = [key], [val]
    for _ in range(2):
        keys.append(moved(keys[-1], block_before))
        vals.append(moved(vals[-1], block_before))
    (q,) = project(*shared, (query_gain * QUERY_SCALE)[None], cos, sin, 0, (True, True))
    mixed = exchanged(attend(block[None], q, keys, vals), OCTANT)

    branch, sums = token_sums(mixed, out_weights, out_gains, h_share, 4)
    sums = exchanged(sums, ("xh", "xl"))
    values = partial_values(sums, branch, out_gains, h_share, 16)
    values = exchanged(values, OCTANT + ("core",)).reshape(4, 2, 2, rows).sum(axis=0)
    pos = pos.reshape(2, 1, rows)
    values = jnp.where(pos < lengths[None, :, None], values, 0.0)
    reward = jnp.sum(jnp.where(pos == reward_pos[None, :, None], values, 0.0), axis=(0, 2))
    reward = told_to_all(reward, ("z", "yy")).sum(axis=0)
    token_values = lax.dynamic_index_in_dim(values, parity, 0, keepdims=False)
    token_values = lax.dynamic_slice_in_dim(token_values, half * tok_dev, tok_dev, 1)
    return token_values, reward


def solution(mesh):
    torus = Mesh(mesh.devices.reshape(SIZES), AXES)
    in_specs = (
        P(None, SEQ, None),
        P(),
        P(),
        P(SEQ),
        P(SEQ, SECTION),
        P(SEQ, SECTION),
        P(SEQ, SECTION),
        P(),
        P(),
        P(SECTION, SEQ),
        P(SEQ),
        P(SEQ),
        P(SEQ),
    )
    out_specs = (P(None, SEQ), P())

    return jax.shard_map(local, mesh=torus, in_specs=in_specs, out_specs=out_specs, check_vma=False)
```

```python
import jax
import jax.numpy as jnp
import numpy as np
from jax import lax
from jax.experimental import pallas as pl
from jax.experimental.pallas import tpu as pltpu
from jax.sharding import Mesh
from jax.sharding import PartitionSpec as P


HD = 128
GROUP = 2
NORM_EPS = 1e-06
QUERY_SCALE = 168.0 ** (-0.5)
ROPE_BASE = 10000.0
SIZES = (2, 2, 8, 4, 2, 2)
AXES = ("xh", "core", "z", "yy", "p", "xl")
SECTION = ("xh", "core")
SEQ = ("z", "yy", "p", "xl")
AXIS_Y = ("yy", "p")
OCTANT = ("xh", "xl", "p")
NT = (((1,), (1,)), ((), ()))


def pairs_of(source_of):
    out = []
    for there in np.ndindex(*SIZES):
        here = source_of(*there)
        if here is not None:
            out.append(
                (int(np.ravel_multi_index(here, SIZES)), int(np.ravel_multi_index(there, SIZES)))
            )
    return out


def row_source(xh, c, z, yy, p, l):
    return (xh, l, z, 2 * c + yy // 2, yy % 2, p)


def out_source(xh, c, z, yy, p, l):
    s, o = divmod(2 * z + c, 4)
    q = 32 * (2 * xh + l) + 8 * o + 2 * yy + p
    return (s // 2, s % 2, q // 16, (q // 4) % 4, (q // 2) % 2, q % 2)


def beside(across_p, across_l):
    return lambda xh, c, z, yy, p, l: (xh, c, z, yy, p ^ across_p, l ^ across_l)


def block_before(xh, c, z, yy, p, l):
    block = 4 * z + yy - 1
    return None if block < 0 else (xh, c, block // 4, block % 4, p, l)


def moved(array, source_of):
    return lax.ppermute(array, AXES, pairs_of(source_of))


def told_to_all(array, axes):
    n = lax.axis_size(axes)
    return lax.all_to_all(jnp.broadcast_to(array[None], (n, *array.shape)), axes, 0, 0, tiled=True)


def exchanged(tiles, axes):
    return lax.all_to_all(tiles, axes, 0, 0, tiled=True)


def rms_rows(piece, gain):
    wide = piece.astype(jnp.float32)
    inverse = lax.rsqrt(jnp.mean(wide * wide, axis=1, keepdims=True) + NORM_EPS)
    return (wide * inverse * gain).astype(jnp.bfloat16)


def norm_kernel(order_ref, gain_ref, *refs):
    out_ref = refs[3]
    for k in range(4):
        rows = refs[0].shape[0]
        at = pl.multiple_of(order_ref[k] * rows, rows)
        if k < 3:
            out_ref[pl.ds(at, rows), :] = rms_rows(refs[k][...], gain_ref[...])
        else:
            out_ref[pl.ds(at, rows), :] = jnp.zeros((rows, out_ref.shape[1]), jnp.bfloat16)


def normed_rows(order, gain, pieces):
    rows, width = pieces[0].shape
    vmem = pl.BlockSpec(memory_space=pltpu.VMEM)
    return pl.pallas_call(
        norm_kernel,
        in_specs=[pl.BlockSpec(memory_space=pltpu.SMEM)] + [vmem] * 4,
        out_specs=vmem,
        out_shape=jax.ShapeDtypeStruct((4 * rows, width), jnp.bfloat16),
        name="norm",
    )(order, gain, *pieces)


def project_kernel(turns, order_ref, rows_ref, last_ref, in_gain_ref, w_ref, *refs):
    gain_ref, cos_ref, sin_ref = refs[:3]
    outs, normed_ref = refs[3:-1], refs[-1]
    j = pl.program_id(0)
    rows = last_ref.shape[0]
    at = pl.multiple_of(order_ref[3] * rows, rows)

    @pl.when(j == 0)
    def _():
        normed_ref[...] = rms_rows(last_ref[...], in_gain_ref[...])

    acc = jnp.dot(rows_ref[...], w_ref[...], preferred_element_type=jnp.float32)
    last = jnp.dot(normed_ref[...], w_ref[...], preferred_element_type=jnp.float32)

    def turned(tile, cos, sin):
        unit = tile * lax.rsqrt(jnp.mean(tile * tile, axis=1, keepdims=True) + NORM_EPS)
        unit = unit * gain_ref[...]
        return unit * cos + pltpu.roll(unit, HD // 2, 1) * sin

    def store(out_ref, turn):
        if turn:
            out_ref[...] = turned(acc, cos_ref[...], sin_ref[...]).astype(jnp.bfloat16)
            there = turned(last, cos_ref[pl.ds(at, rows), :], sin_ref[pl.ds(at, rows), :])
        else:
            out_ref[...] = acc.astype(jnp.bfloat16)
            there = last
        out_ref[pl.ds(at, rows), :] = there.astype(jnp.bfloat16)

    if len(outs) == 1:
        store(outs[0], True)
    else:
        for k in range(2):
            pl.when(j == k)(lambda k=k: store(outs[k], turns[k]))


def project(order, normed, last, in_gain, weights, gain, cos, sin, first, turns):
    rows, width = normed.shape
    vmem = pl.BlockSpec(memory_space=pltpu.VMEM)
    if turns[1]:
        out_specs = [pl.BlockSpec((rows, HD), lambda j: (0, j))]
        out_shape = [jax.ShapeDtypeStruct((rows, 2 * HD), jnp.bfloat16)]
    else:
        out_specs = [pl.BlockSpec((rows, HD), lambda j: (0, 0))] * 2
        out_shape = [jax.ShapeDtypeStruct((rows, HD), jnp.bfloat16)] * 2
    return pl.pallas_call(
        lambda *refs: project_kernel(turns, *refs),
        grid=(2,),
        in_specs=[
            pl.BlockSpec(memory_space=pltpu.SMEM),
            vmem,
            vmem,
            vmem,
            pl.BlockSpec((width, HD), lambda j: (0, j + first)),
            vmem,
            vmem,
            vmem,
        ],
        out_specs=out_specs,
        out_shape=out_shape,
        scratch_shapes=[pltpu.VMEM(last.shape, jnp.bfloat16)],
        name="project",
    )(order, normed, last, in_gain, weights, gain, cos, sin)


def part_of(ref, i, rows):
    return ref[i * rows : (i + 1) * rows, :]


def scores_of(q, k, place, block, query, key):
    s = lax.dot_general(q, k, NT, preferred_element_type=jnp.float32)
    a, i = place
    if i - a == 4:
        return jnp.where(key <= query, s, -1e30)
    if i >= 4:
        return s
    there = 2 * block + (i - 4) >= 0
    if i == a:
        return jnp.where((key > query) & there, s, -1e30)
    return jnp.where(there, s, -1e30)


def row_max(scores):
    top = jnp.max(scores[0], axis=1, keepdims=True)
    for s in scores[1:]:
        top = jnp.maximum(top, jnp.max(s, axis=1, keepdims=True))
    return top


def attend_kernel(block_ref, q_ref, *refs):
    keys, vals, out_ref = refs[2::-1], refs[5:2:-1], refs[6]
    rows = q_ref.shape[0] // 2
    query = lax.broadcasted_iota(jnp.int32, (rows, rows), 0)
    key = lax.broadcasted_iota(jnp.int32, (rows, rows), 1)
    for a in range(2):
        at = slice(a * rows, (a + 1) * rows)
        pieces = range(a, a + 5)
        for g in range(GROUP):
            wide = slice(g * HD, (g + 1) * HD)
            q = q_ref[at, wide]
            scores = [
                scores_of(q, part_of(keys[i // 2], i % 2, rows), (a, i), block_ref[0], query, key)
                for i in pieces
            ]
            top = row_max(scores)
            terms = [jnp.exp(s - top) for s in scores]
            total = sum(jnp.sum(e, axis=1, keepdims=True) for e in terms)
            share = 1.0 / total
            mixed = sum(
                jnp.dot(
                    (e * share).astype(jnp.bfloat16),
                    part_of(vals[i // 2], i % 2, rows),
                    preferred_element_type=jnp.float32,
                )
                for e, i in zip(terms, pieces)
            ).astype(jnp.bfloat16)
            for x in range(4):
                out_ref[2 * x + a, :, wide] = mixed


def attend(block, q, keys, vals):
    rows, wide = q.shape
    vmem = pl.BlockSpec(memory_space=pltpu.VMEM)
    return pl.pallas_call(
        attend_kernel,
        in_specs=[pl.BlockSpec(memory_space=pltpu.SMEM)] + [vmem] * 7,
        out_specs=vmem,
        out_shape=jax.ShapeDtypeStruct((8, rows // 2, wide), jnp.bfloat16),
        name="attend",
    )(block, q, *keys, *vals)


def sums_kernel(mixed_ref, w_ref, gains_ref, h_ref, out_ref, sums_ref):
    o = pl.program_id(0)

    @pl.when(o == 0)
    def _():
        sums_ref[...] = jnp.zeros_like(sums_ref)

    wide = mixed_ref.shape[2]
    branch = 0.0
    for head in range(8):
        at = (head % 2) * wide
        branch = branch + lax.dot_general(
            w_ref[head // 2, 0, :, at : at + wide],
            mixed_ref[head],
            NT,
            preferred_element_type=jnp.float32,
        )
    gains = gains_ref[0]
    post, final, head = gains[:, 0:1], gains[:, 1:2], gains[:, 2:3]
    read = final * head
    hidden = h_ref[0].astype(jnp.float32)
    scaled = branch * post
    for k, term in enumerate(
        (
            branch * branch,
            scaled * scaled,
            hidden * scaled,
            scaled * read,
            hidden * read,
            hidden * hidden,
        )
    ):
        sums_ref[k : k + 1, :] += jnp.sum(term, axis=0, keepdims=True)

    @pl.when(o == pl.num_programs(0) - 1)
    def _():
        for k in range(out_ref.shape[0]):
            out_ref[k] = sums_ref[...]


def token_sums(mixed, weights, gains, h_share, copies):
    rows = mixed.shape[1]
    _, parts, depth, wide = weights.shape
    return pl.pallas_call(
        sums_kernel,
        grid=(parts,),
        in_specs=[
            pl.BlockSpec(memory_space=pltpu.VMEM),
            pl.BlockSpec((4, 1, depth, wide), lambda o: (0, o, 0, 0)),
            pl.BlockSpec((1, depth, 3), lambda o: (o, 0, 0)),
            pl.BlockSpec((1, depth, rows), lambda o: (o, 0, 0)),
        ],
        out_specs=pl.BlockSpec((copies, 8, rows), lambda o: (0, 0, 0)),
        out_shape=jax.ShapeDtypeStruct((copies, 8, rows), jnp.float32),
        scratch_shapes=[pltpu.VMEM((8, rows), jnp.float32)],
        name="token_sums",
    )(mixed, weights, gains, h_share)


def local(
    hidden,
    lengths,
    reward_pos,
    in_gain,
    w_query,
    w_key,
    w_value,
    query_gain,
    key_gain,
    w_out,
    post_gain,
    final_gain,
    value_head,
):
    _, tok_dev, width = hidden.shape
    shard = in_gain.shape[0]
    octet_rows = 8 * shard
    rows = 2 * tok_dev
    block = 4 * lax.axis_index("z") + lax.axis_index("yy")
    parity, half = lax.axis_index("p"), lax.axis_index("xl")
    place = 2 * lax.axis_index("xh") + half

    def with_row(tile, values):
        return jnp.concatenate([tile, jnp.pad(values, (0, 4 * HD - values.shape[0]))[None]], axis=0)

    heads = [
        with_row(
            jnp.concatenate(
                [
                    w_query[:, 2 * k * HD : 2 * (k + 1) * HD],
                    w_key[:, k * HD : (k + 1) * HD],
                    w_value[:, k * HD : (k + 1) * HD],
                ],
                axis=1,
            ),
            in_gain,
        )
        for k in range(2)
    ]
    out_shard = with_row(w_out.T, jnp.concatenate([post_gain, final_gain, value_head]))
    heads = moved(jnp.stack(heads), row_source)
    out_shard = moved(out_shard, out_source)
    tiles = jnp.concatenate(
        [jnp.tile(heads, (4, 1, 1)), jnp.broadcast_to(out_shard, (8, *out_shard.shape))], axis=2
    )
    octet = exchanged(tiles, AXIS_Y)
    gains = [octet[:, shard, at : at + shard] for at in (0, *range(4 * HD, 4 * HD + 3 * shard, shard))]
    gains = jnp.stack(gains).reshape(4, octet_rows)
    gains = jnp.pad(gains, ((0, 0), (0, 256 - octet_rows)))
    octet = octet[:, :shard].reshape(octet_rows, 8 * HD)
    weights = lax.all_gather(octet[:, : 4 * HD], ("z", "core"), axis=0, tiled=True)
    out_weights = lax.all_gather(octet[:, 4 * HD :], ("z", "core"), axis=0, tiled=True)
    out_weights = out_weights.reshape(4, 4, octet_rows, -1)
    gains = told_to_all(gains, ("z", "core"))
    gains = gains[:, :, :octet_rows].astype(jnp.float32)
    in_full = gains[:, 0].reshape(1, width)
    out_gains = gains[:4, 1:].swapaxes(1, 2)

    mine = lax.dynamic_index_in_dim(hidden, lax.axis_index("core"), 0, keepdims=False)
    near = moved(mine, beside(0, 1))
    far = [moved(mine, beside(1, 0))]
    far.append(moved(mine, beside(1, 1)))
    pieces = (mine, near, *far)
    order = jnp.stack(
        [
            2 * parity + half,
            2 * parity + 1 - half,
            2 - 2 * parity + half,
            2 - 2 * parity + 1 - half,
        ]
    )
    normed = normed_rows(order, in_full, pieces[:3])
    h_share = jnp.concatenate(
        [jnp.where(half == 0, mine, near), jnp.where(half == 0, near, mine)], axis=0
    )
    h_share = lax.dynamic_slice_in_dim(h_share, place * (width // 4), width // 4, 1)
    h_share = h_share.T.reshape(4, octet_rows, rows)

    pos = block * 2 * rows + jnp.arange(2 * rows, dtype=jnp.int32)
    frequency = (ROPE_BASE ** (-np.arange(HD // 2) * 2.0 / HD)).astype(np.float32)
    angles = pos.astype(jnp.float32)[:, None] * frequency[None, :]
    cos, sin = jnp.cos(angles), jnp.sin(angles)
    cos = jnp.concatenate([cos, cos], axis=1)
    sin = jnp.concatenate([-sin, sin], axis=1)

    shared = (order, normed, pieces[3], in_full, weights)
    key, val = project(*shared, key_gain[None], cos, sin, 2, (True, False))
    keys, vals = [key], [val]
    for _ in range(2):
        keys.append(moved(keys[-1], block_before))
        vals.append(moved(vals[-1], block_before))
    (q,) = project(*shared, (query_gain * QUERY_SCALE)[None], cos, sin, 0, (True, True))
    mixed = exchanged(attend(block[None], q, keys, vals), OCTANT)

    sums = exchanged(token_sums(mixed, out_weights, out_gains, h_share, 16), OCTANT + ("core",))
    sums = sums.reshape(4, 2, 2, 8, rows).sum(axis=0)
    branch_sq, scaled_sq, cross, read_branch, read_hidden, hidden_sq = (
        sums[:, :, k] for k in range(6)
    )
    scale = lax.rsqrt(branch_sq / width + NORM_EPS)
    residual_sq = hidden_sq + scale * (2.0 * cross + scale * scaled_sq)
    residual_sq = jnp.maximum(residual_sq, 0.0)
    values = (read_hidden + scale * read_branch) * lax.rsqrt(residual_sq / width + NORM_EPS)
    pos = pos.reshape(2, 1, rows)
    values = jnp.where(pos < lengths[None, :, None], values, 0.0)
    reward = jnp.sum(jnp.where(pos == reward_pos[None, :, None], values, 0.0), axis=(0, 2))
    reward = told_to_all(reward, ("z", "yy")).sum(axis=0)
    token_values = lax.dynamic_index_in_dim(values, parity, 0, keepdims=False)
    token_values = lax.dynamic_slice_in_dim(token_values, half * tok_dev, tok_dev, 1)
    return token_values, reward


def solution(mesh):
    torus = Mesh(mesh.devices.reshape(SIZES), AXES)
    in_specs = (
        P(None, SEQ, None),
        P(),
        P(),
        P(SEQ),
        P(SEQ, SECTION),
        P(SEQ, SECTION),
        P(SEQ, SECTION),
        P(),
        P(),
        P(SECTION, SEQ),
        P(SEQ),
        P(SEQ),
        P(SEQ),
    )
    out_specs = (P(None, SEQ), P())

    return jax.shard_map(local, mesh=torus, in_specs=in_specs, out_specs=out_specs, check_vma=False)
```

```python
import jax
import jax.numpy as jnp
import numpy as np
from jax import lax
from jax.experimental import pallas as pl
from jax.experimental.pallas import tpu as pltpu
from jax.sharding import Mesh
from jax.sharding import PartitionSpec as P


HD = 128
GROUP = 2
NORM_EPS = 1e-06
QUERY_SCALE = 168.0 ** (-0.5)
ROPE_BASE = 10000.0
SIZES = (2, 2, 8, 4, 2, 2)
AXES = ("xh", "core", "z", "yy", "p", "xl")
SECTION = ("xh", "core")
SEQ = ("z", "yy", "p", "xl")
AXIS_Y = ("yy", "p")
OCTANT = ("xh", "xl", "p")
NT = (((1,), (1,)), ((), ()))


def pairs_of(source_of):
    out = []
    for there in np.ndindex(*SIZES):
        here = source_of(*there)
        if here is not None:
            out.append(
                (int(np.ravel_multi_index(here, SIZES)), int(np.ravel_multi_index(there, SIZES)))
            )
    return out


def row_source(xh, c, z, yy, p, l):
    return (xh, l, z, 2 * c + yy // 2, yy % 2, p)


def out_source(xh, c, z, yy, p, l):
    s, o = divmod(2 * z + c, 4)
    q = 32 * (2 * xh + l) + 8 * o + 2 * yy + p
    return (s // 2, s % 2, q // 16, (q // 4) % 4, (q // 2) % 2, q % 2)


def beside(across_p, across_l):
    return lambda xh, c, z, yy, p, l: (xh, c, z, yy, p ^ across_p, l ^ across_l)


def block_before(xh, c, z, yy, p, l):
    block = 4 * z + yy - 1
    return None if block < 0 else (xh, c, block // 4, block % 4, p, l)


def moved(array, source_of):
    return lax.ppermute(array, AXES, pairs_of(source_of))


def told_to_all(array, axes):
    n = lax.axis_size(axes)
    return lax.all_to_all(jnp.broadcast_to(array[None], (n, *array.shape)), axes, 0, 0, tiled=True)


def exchanged(tiles, axes):
    return lax.all_to_all(tiles, axes, 0, 0, tiled=True)


def norm_kernel(order_ref, gain_ref, *refs):
    for k in range(4):
        wide = refs[k][...].astype(jnp.float32)
        inverse = lax.rsqrt(jnp.mean(wide * wide, axis=1, keepdims=True) + NORM_EPS)
        rows = wide.shape[0]
        at = pl.multiple_of(order_ref[k] * rows, rows)
        refs[4][pl.ds(at, rows), :] = (wide * inverse * gain_ref[...]).astype(jnp.bfloat16)


def normed_rows(order, gain, pieces):
    rows, width = pieces[0].shape
    vmem = pl.BlockSpec(memory_space=pltpu.VMEM)
    return pl.pallas_call(
        norm_kernel,
        in_specs=[pl.BlockSpec(memory_space=pltpu.SMEM)] + [vmem] * 5,
        out_specs=vmem,
        out_shape=jax.ShapeDtypeStruct((4 * rows, width), jnp.bfloat16),
        name="norm",
    )(order, gain, *pieces)


def project_kernel(turned_heads, rows_ref, w_ref, gain_ref, cos_ref, sin_ref, out_ref):
    acc = jnp.dot(rows_ref[...], w_ref[...], preferred_element_type=jnp.float32)

    def turn():
        unit = acc * lax.rsqrt(jnp.mean(acc * acc, axis=1, keepdims=True) + NORM_EPS)
        unit = unit * gain_ref[...]
        other = pltpu.roll(unit, HD // 2, 1)
        out_ref[...] = (unit * cos_ref[...] + other * sin_ref[...]).astype(jnp.bfloat16)

    if turned_heads == 2:
        turn()
    else:
        pl.when(pl.program_id(0) == 0)(turn)

        @pl.when(pl.program_id(0) == 1)
        def _():
            out_ref[...] = acc.astype(jnp.bfloat16)


def project(normed, weights, gain, cos, sin, first, turned_heads):
    rows, width = normed.shape
    vmem = pl.BlockSpec(memory_space=pltpu.VMEM)
    return pl.pallas_call(
        lambda *refs: project_kernel(turned_heads, *refs),
        grid=(2,),
        in_specs=[
            vmem,
            pl.BlockSpec((width, HD), lambda j: (0, j + first)),
            vmem,
            vmem,
            vmem,
        ],
        out_specs=pl.BlockSpec((rows, HD), lambda j: (0, j)),
        out_shape=jax.ShapeDtypeStruct((rows, 2 * HD), jnp.bfloat16),
        name="project",
    )(normed, weights, gain, cos, sin)


def attend_kernel(block_ref, q_ref, own_ref, back1_ref, back2_ref, out_ref):
    held = (back2_ref, back1_ref, own_ref)
    rows = q_ref.shape[0] // 2
    block = block_ref[0]
    query = lax.broadcasted_iota(jnp.int32, (rows, rows), 0)
    key = lax.broadcasted_iota(jnp.int32, (rows, rows), 1)
    for a in range(2):
        pieces = [
            held[i // 2][(i % 2) * rows : (i % 2 + 1) * rows, :] for i in range(a, a + 5)
        ]
        for g in range(GROUP):
            q = q_ref[a * rows : (a + 1) * rows, g * HD : (g + 1) * HD]
            scores = []
            for k, piece in enumerate(pieces):
                s = lax.dot_general(q, piece[:, :HD], NT, preferred_element_type=jnp.float32)
                there = 2 * block + (a + k - 4) >= 0
                if k == 4:
                    s = jnp.where(key <= query, s, -1e30)
                elif k == 0:
                    s = jnp.where((key > query) & there, s, -1e30)
                elif a + k < 4:
                    s = jnp.where(there, s, -1e30)
                scores.append(s)
            top = jnp.max(scores[0], axis=1, keepdims=True)
            for s in scores[1:]:
                top = jnp.maximum(top, jnp.max(s, axis=1, keepdims=True))
            terms = [jnp.exp(s - top) for s in scores]
            share = 1.0 / sum(jnp.sum(e, axis=1, keepdims=True) for e in terms)
            mixed = 0.0
            for e, piece in zip(terms, pieces):
                mixed = mixed + jnp.dot(
                    (e * share).astype(jnp.bfloat16),
                    piece[:, HD:],
                    preferred_element_type=jnp.float32,
                )
            mixed = mixed.astype(jnp.bfloat16)
            for x in range(4):
                out_ref[2 * x + a, :, g * HD : (g + 1) * HD] = mixed


def attend(block, q, held):
    rows, wide = q.shape
    vmem = pl.BlockSpec(memory_space=pltpu.VMEM)
    return pl.pallas_call(
        attend_kernel,
        in_specs=[pl.BlockSpec(memory_space=pltpu.SMEM)] + [vmem] * 4,
        out_specs=vmem,
        out_shape=jax.ShapeDtypeStruct((8, rows // 2, wide), jnp.bfloat16),
        name="attend",
    )(block, q, *held)


def sums_kernel(mixed_ref, w_ref, gains_ref, h_ref, out_ref, sums_ref):
    o = pl.program_id(0)

    @pl.when(o == 0)
    def _():
        sums_ref[...] = jnp.zeros_like(sums_ref)

    wide = mixed_ref.shape[2]
    branch = 0.0
    for head in range(8):
        at = (head % 2) * wide
        branch = branch + lax.dot_general(
            w_ref[head // 2, 0, :, at : at + wide],
            mixed_ref[head],
            NT,
            preferred_element_type=jnp.float32,
        )
    gains = gains_ref[0]
    post, final, head = gains[:, 0:1], gains[:, 1:2], gains[:, 2:3]
    read = final * head
    hidden = h_ref[0].astype(jnp.float32)
    scaled = branch * post
    for k, term in enumerate(
        (
            branch * branch,
            scaled * scaled,
            hidden * scaled,
            scaled * read,
            hidden * read,
            hidden * hidden,
        )
    ):
        sums_ref[k : k + 1, :] += jnp.sum(term, axis=0, keepdims=True)

    @pl.when(o == pl.num_programs(0) - 1)
    def _():
        for k in range(out_ref.shape[0]):
            out_ref[k] = sums_ref[...]


def token_sums(mixed, weights, gains, h_share, copies):
    rows = mixed.shape[1]
    _, parts, depth, wide = weights.shape
    return pl.pallas_call(
        sums_kernel,
        grid=(parts,),
        in_specs=[
            pl.BlockSpec(memory_space=pltpu.VMEM),
            pl.BlockSpec((4, 1, depth, wide), lambda o: (0, o, 0, 0)),
            pl.BlockSpec((1, depth, 3), lambda o: (o, 0, 0)),
            pl.BlockSpec((1, depth, rows), lambda o: (o, 0, 0)),
        ],
        out_specs=pl.BlockSpec((copies, 8, rows), lambda o: (0, 0, 0)),
        out_shape=jax.ShapeDtypeStruct((copies, 8, rows), jnp.float32),
        scratch_shapes=[pltpu.VMEM((8, rows), jnp.float32)],
        name="token_sums",
    )(mixed, weights, gains, h_share)


def local(
    hidden,
    lengths,
    reward_pos,
    in_gain,
    w_query,
    w_key,
    w_value,
    query_gain,
    key_gain,
    w_out,
    post_gain,
    final_gain,
    value_head,
):
    _, tok_dev, width = hidden.shape
    shard = in_gain.shape[0]
    octet_rows = 8 * shard
    rows = 2 * tok_dev
    block = 4 * lax.axis_index("z") + lax.axis_index("yy")
    parity, half = lax.axis_index("p"), lax.axis_index("xl")
    place = 2 * lax.axis_index("xh") + half

    def with_row(tile, values):
        return jnp.concatenate([tile, jnp.pad(values, (0, 4 * HD - values.shape[0]))[None]], axis=0)

    heads = [
        with_row(
            jnp.concatenate(
                [
                    w_query[:, 2 * k * HD : 2 * (k + 1) * HD],
                    w_key[:, k * HD : (k + 1) * HD],
                    w_value[:, k * HD : (k + 1) * HD],
                ],
                axis=1,
            ),
            in_gain,
        )
        for k in range(2)
    ]
    out_shard = with_row(w_out.T, jnp.concatenate([post_gain, final_gain, value_head]))
    heads = moved(jnp.stack(heads), row_source)
    out_shard = moved(out_shard, out_source)
    tiles = jnp.concatenate(
        [jnp.tile(heads, (4, 1, 1)), jnp.broadcast_to(out_shard, (8, *out_shard.shape))], axis=2
    )
    octet = exchanged(tiles, AXIS_Y)
    gains = [octet[:, shard, at : at + shard] for at in (0, *range(4 * HD, 4 * HD + 3 * shard, shard))]
    gains = jnp.stack(gains).reshape(4, octet_rows)
    gains = jnp.pad(gains, ((0, 0), (0, 256 - octet_rows)))
    octet = octet[:, :shard].reshape(octet_rows, 8 * HD)
    weights = lax.all_gather(octet[:, : 4 * HD], ("z", "core"), axis=0, tiled=True)
    out_weights = lax.all_gather(octet[:, 4 * HD :], ("z", "core"), axis=0, tiled=True)
    out_weights = out_weights.reshape(4, 4, octet_rows, -1)
    gains = told_to_all(gains, ("z", "core"))
    gains = gains[:, :, :octet_rows].astype(jnp.float32)
    in_full = gains[:, 0].reshape(1, width)
    out_gains = gains[:4, 1:].swapaxes(1, 2)

    mine = lax.dynamic_index_in_dim(hidden, lax.axis_index("core"), 0, keepdims=False)
    near = moved(mine, beside(0, 1))
    far = moved(mine, beside(1, 0)), moved(mine, beside(1, 1))
    pieces = (mine, near, *far)
    order = jnp.stack(
        [
            2 * parity + half,
            2 * parity + 1 - half,
            2 - 2 * parity + half,
            2 - 2 * parity + 1 - half,
        ]
    )
    normed = normed_rows(order, in_full, pieces)
    h_share = jnp.concatenate(
        [jnp.where(half == 0, mine, near), jnp.where(half == 0, near, mine)], axis=0
    )
    h_share = lax.dynamic_slice_in_dim(h_share, place * (width // 4), width // 4, 1)
    h_share = h_share.T.reshape(4, octet_rows, rows)

    pos = block * 2 * rows + jnp.arange(2 * rows, dtype=jnp.int32)
    frequency = (ROPE_BASE ** (-np.arange(HD // 2) * 2.0 / HD)).astype(np.float32)
    angles = pos.astype(jnp.float32)[:, None] * frequency[None, :]
    cos, sin = jnp.cos(angles), jnp.sin(angles)
    cos = jnp.concatenate([cos, cos], axis=1)
    sin = jnp.concatenate([-sin, sin], axis=1)

    held = [project(normed, weights, key_gain[None], cos, sin, 2, 1)]
    for _ in range(2):
        held.append(moved(held[-1], block_before))
    q = project(normed, weights, (query_gain * QUERY_SCALE)[None], cos, sin, 0, 2)
    mixed = exchanged(attend(block[None], q, held), OCTANT)

    sums = exchanged(token_sums(mixed, out_weights, out_gains, h_share, 16), OCTANT + ("core",))
    sums = sums.reshape(4, 2, 2, 8, rows).sum(axis=0)
    branch_sq, scaled_sq, cross, read_branch, read_hidden, hidden_sq = (
        sums[:, :, k] for k in range(6)
    )
    scale = lax.rsqrt(branch_sq / width + NORM_EPS)
    residual_sq = hidden_sq + scale * (2.0 * cross + scale * scaled_sq)
    residual_sq = jnp.maximum(residual_sq, 0.0)
    values = (read_hidden + scale * read_branch) * lax.rsqrt(residual_sq / width + NORM_EPS)
    pos = pos.reshape(2, 1, rows)
    values = jnp.where(pos < lengths[None, :, None], values, 0.0)
    reward = jnp.sum(jnp.where(pos == reward_pos[None, :, None], values, 0.0), axis=(0, 2))
    reward = told_to_all(reward, ("z", "yy")).sum(axis=0)
    token_values = lax.dynamic_index_in_dim(values, parity, 0, keepdims=False)
    token_values = lax.dynamic_slice_in_dim(token_values, half * tok_dev, tok_dev, 1)
    return token_values, reward


def solution(mesh):
    torus = Mesh(mesh.devices.reshape(SIZES), AXES)
    in_specs = (
        P(None, SEQ, None),
        P(),
        P(),
        P(SEQ),
        P(SEQ, SECTION),
        P(SEQ, SECTION),
        P(SEQ, SECTION),
        P(),
        P(),
        P(SECTION, SEQ),
        P(SEQ),
        P(SEQ),
        P(SEQ),
    )
    out_specs = (P(None, SEQ), P())

    return jax.shard_map(local, mesh=torus, in_specs=in_specs, out_specs=out_specs, check_vma=False)
```
